32 devices in a mesh: seq: 8 (over z, y), head: 4 (over x, core).
Axes of the slice: x: 2, y: 2, z: 4, core: 2. Of those that a mesh axis runs over, the one named last changes fastest.
Arguments:
- queries: bfloat16 [2048, 4096], P('seq', 'head'), may hold values from -8 to 8
- self_keys: bfloat16 [2048, 1024], P('seq', 'head'), may hold values from -6 to 6
- self_values: bfloat16 [2048, 1024], P('seq', 'head'), may hold values from -6 to 6
- store_keys: bfloat16 [32768, 1024], P('seq', 'head'), may hold values from -6 to 6
- store_values: bfloat16 [32768, 1024], P('seq', 'head'), may hold values from -6 to 6
- kv_slot: int32 [256], replicated, may hold values from 0 to 255, as said below
- neighbours: int32 [16, 64], P('seq'), may hold values from 0 to 255, as said below
- counts: int32 [16], P('seq'), may hold values from 1 to 64, 96 in all
- out_weight: bfloat16 [4096, 4096], P('head', 'seq'), may hold values from -0.375 to 0.375
Outputs:
- mixed: bfloat16 [2048, 4096], P(('seq', 'head'))
The draws below stay inside these ranges and needn't reach their ends.
Inputs may be any that keep to these rules, and one draw needn't show every extreme that they name: A permutation of the store blocks: block b is stored at slot kv_slot[b], on index kv_slot[b] // 32 of seq. `neighbours`: each row names 64 different store blocks in no particular order; only entries e < counts of the row are listed, the rest is padding. Counting by the index of seq on which a block is stored, each row names exactly 8 blocks on every index, and the 2 rows of one index of seq name the same single block on every index of seq.
All inputs are finite; a program needn't handle non-finite values. No bound on the sum of `counts` on one device may be relied on, other than what follows from the above.
Results may differ from the reference program's by a relative error of at most 0.012.
Values may be sent and summed in bfloat16 or wider, within the bound.
A program may use at most 128 MiB of HBM per device.

```python
import math
import jax
import jax.numpy as jnp
import numpy as np
from jax import lax

D = 4096
H = 32
KVH = 8
DH = 128
BLK = 128
DEG = 64
MEAN_DEG = 6
QB_DEV = 2
KB_DEV = 32
NQB = 16
NKB = 256
TOKENS = 2048
STORE_TOKENS = 32768
CAPQ = 8
CAP = 8
N_SEQ = 8


def graph_tables(key):
    slot_scores = jax.random.randint(jax.random.fold_in(key, 101), (NKB,), 0, 1 << 16) * NKB + jnp.arange(NKB)
    kv_slot = jnp.argsort(slot_scores).astype(jnp.int32)
    stored_at = jnp.argsort(kv_slot).astype(jnp.int32)
    pick_scores = jax.random.randint(jax.random.fold_in(key, 102), (N_SEQ, N_SEQ, KB_DEV), 0, 1 << 16) * KB_DEV + jnp.arange(KB_DEV)
    kept_picks = jnp.argsort(pick_scores, axis=-1)[:, :, :CAP]
    block_ids = jnp.arange(NQB)
    position = block_ids % QB_DEV
    holder = block_ids // QB_DEV
    random_start = jax.random.randint(jax.random.fold_in(key, 103), (NQB, N_SEQ), 0, CAP)
    forced = position * CAPQ
    starting = jnp.where((forced < CAP)[:, None], forced[:, None], random_start)
    offsets = (starting[:, :, None] + jnp.arange(CAPQ)[None, None, :]) % CAP
    within = jnp.take_along_axis(kept_picks[holder], offsets, axis=-1)
    slot_ids = (jnp.arange(N_SEQ)[None, :, None] * KB_DEV + within).reshape(NQB, DEG)
    order_scores = jax.random.randint(jax.random.fold_in(key, 104), (NQB, DEG), 0, 1 << 16) * DEG + jnp.arange(DEG)
    ordering = jnp.argsort(order_scores, axis=-1)
    slot_ids = jnp.take_along_axis(slot_ids, ordering, axis=-1)
    return (kv_slot, stored_at[slot_ids].astype(jnp.int32))


def draw_kv_slot(key, part):
    return graph_tables(key)[0]


def draw_neighbours(key, part):
    return graph_tables(key)[1]


def draw_queries(key, part):
    drawn = 2.0 * jax.random.truncated_normal(jax.random.fold_in(key, 1), -4.0, 4.0, (TOKENS, H * DH), jnp.float32)
    return drawn.astype(jnp.bfloat16)


def draw_self_keys(key, part):
    drawn = jax.random.truncated_normal(jax.random.fold_in(key, 2), -6.0, 6.0, (TOKENS, KVH * DH), jnp.float32)
    return drawn.astype(jnp.bfloat16)


def block_levels(own_key, shape, cuts, low, largest):
    level, own = 1.0, jax.random.fold_in(own_key, 6)
    for axis_at, blocks in cuts:
        steps = jnp.exp(jax.random.uniform(jax.random.fold_in(own, axis_at), (blocks,), jnp.float32, low / len(cuts), largest / len(cuts)))
        level = level * jnp.repeat(steps, shape[axis_at] // blocks).reshape([-1 if axis == axis_at else 1 for axis in range(len(shape))])
    return level


def profile(number_of, total, most, lean):
    loads = [(1 << 20) // math.isqrt(grade ** lean) + 1 for grade in range(2, number_of + 1)]
    spare, given = total - most - (number_of - 1), [1] * (number_of - 1)
    while spare > 0:
        candidates = [i for i in range(number_of - 1) if given[i] < most]
        whole, remaining = sum([loads[i] for i in candidates]), spare
        for i in candidates:
            more = min(most - given[i], max(1, remaining * loads[i] // whole), spare)
            given[i] = given[i] + more
            spare = spare - more
    return np.array([most] + given)


def ragged_sizes(key, count, total, limit, slope):
    if count == 2:
        one = jax.random.randint(key, (), max(1, total - limit), min(limit, total - 1) + 1)
        return jnp.stack([one, total - one])
    sizes = jnp.asarray(profile(count, total, limit, slope), jnp.int32)
    twos = (count - 1) // 2
    giver, sink = sizes[1:1 + 2 * twos:2], sizes[2:2 + 2 * twos:2]
    slack = jnp.minimum(giver - 1, limit - sink)
    moved = jax.random.randint(jax.random.fold_in(key, 1), (twos,), 0, 1 << 20) % (slack + 1)
    sizes = sizes.at[1:1 + 2 * twos:2].set(giver - moved).at[2:2 + 2 * twos:2].set(sink + moved)
    return sizes[jax.random.permutation(jax.random.fold_in(key, 2), count)]


def scatter_about(key, shape, spread, reach, pieces=(), kind=jnp.bfloat16):
    level = block_levels(key, shape, pieces, -0.22, 0.18) if pieces else 1.0
    values = jax.random.normal(key, shape, jnp.float32) * spread * level
    return jnp.minimum(jnp.maximum(values, -reach), reach).astype(kind)


def setup_inputs(seed: int = 0) -> dict:
    arg_keys = jax.random.split(jax.random.key(seed), 10)
    queries = draw_queries(jax.random.fold_in(arg_keys[9], 71), 0)
    self_keys = draw_self_keys(jax.random.fold_in(arg_keys[9], 71), 0)
    self_values = scatter_about(arg_keys[2], (TOKENS, KVH * DH), 1.0, 6.0, ((0, 8), (1, 4)))
    store_keys = scatter_about(arg_keys[3], (STORE_TOKENS, KVH * DH), 1.0, 6.0, ((0, 8), (1, 4)))
    store_values = scatter_about(arg_keys[4], (STORE_TOKENS, KVH * DH), 1.0, 6.0, ((0, 8), (1, 4)))
    kv_slot = draw_kv_slot(jax.random.fold_in(arg_keys[9], 71), 0)
    neighbours = draw_neighbours(jax.random.fold_in(arg_keys[9], 71), 0)
    counts = ragged_sizes(arg_keys[7], NQB, NQB * MEAN_DEG, DEG, 2).astype(jnp.int32)
    out_weight = scatter_about(arg_keys[8], (H * DH, D), (H * DH // 16) ** -0.5, 0.375, ((0, 4), (1, 8)))
    return dict(queries=queries, self_keys=self_keys, self_values=self_values, store_keys=store_keys, store_values=store_values, kv_slot=kv_slot, neighbours=neighbours, counts=counts, out_weight=out_weight)


def reference(queries, self_keys, self_values, store_keys, store_values, kv_slot, neighbours, counts, out_weight):
    per_group = H // KVH
    scaling = DH ** -0.5
    stored_keys = store_keys.reshape(NKB, BLK, KVH, DH)
    stored_values = store_values.reshape(NKB, BLK, KVH, DH)
    query_blocks = queries.reshape(NQB, BLK, KVH, per_group, DH)
    own_keys = self_keys.reshape(NQB, BLK, KVH, DH)
    own_values = self_values.reshape(NQB, BLK, KVH, DH)
    causal = jnp.arange(BLK)[:, None] >= jnp.arange(BLK)[None, :]

    def rounded(weights):
        return lax.optimization_barrier(weights.astype(jnp.bfloat16)).astype(jnp.float32)

    def one_block(bundle):
        query_rows, near_keys, near_values, adjacency, how_many = bundle
        query_wide = query_rows.astype(jnp.float32)

        def scores_of(key_rows):
            return jnp.einsum("tgrd,ugd->grtu", query_wide, key_rows.astype(jnp.float32)) * scaling

        def fetched(entry):
            slot_id = kv_slot[adjacency[entry]]
            return (lax.dynamic_index_in_dim(stored_keys, slot_id, 0, keepdims=False),
                    lax.dynamic_index_in_dim(stored_values, slot_id, 0, keepdims=False))

        nearby = jnp.where(causal, scores_of(near_keys), -jnp.inf)

        def find_highest(entry, highest):
            return jnp.maximum(highest, jnp.max(scores_of(fetched(entry)[0]), axis=-1))

        highest = lax.fori_loop(jnp.int32(0), how_many, find_highest, jnp.max(nearby, axis=-1))
        near_weights = jnp.exp(nearby - highest[..., None])
        start_sum = jnp.einsum("grtu,ugd->grtd", rounded(near_weights), near_values.astype(jnp.float32))

        def accumulate(entry, carry):
            summed, totals = carry
            key_rows, value_rows = fetched(entry)
            weights = jnp.exp(scores_of(key_rows) - highest[..., None])
            summed = summed + jnp.einsum("grtu,ugd->grtd", rounded(weights), value_rows.astype(jnp.float32))
            return summed, totals + jnp.sum(weights, axis=-1)

        summed, totals = lax.fori_loop(jnp.int32(0), how_many, accumulate, (start_sum, jnp.sum(near_weights, axis=-1)))
        result = summed / totals[..., None]
        return jnp.transpose(result, (2, 0, 1, 3)).reshape(BLK, H * DH).astype(jnp.bfloat16)

    attended = lax.map(one_block, (query_blocks, own_keys, own_values, neighbours, counts))
    attended = attended.reshape(NQB * BLK, H * DH)
    return jnp.dot(attended, out_weight, preferred_element_type=jnp.float32).astype(jnp.bfloat16)
```

```python
import functools

import jax
import jax.numpy as jnp
from jax import lax
from jax.experimental import pallas as pl
from jax.experimental.pallas import tpu as pltpu
from jax.sharding import PartitionSpec as P

H = 32
KVH = 8
DH = 128
BLK = 128
NEG = -1e30
MESH = pl.DeviceIdType.MESH


def part_kernel(
    local_blocks,
    store_blocks,
    slot_ref,
    near_ref,
    count_ref,
    q_ref,
    sk_ref,
    sv_ref,
    k_ref,
    v_ref,
    o_ref,
    lse_ref,
    list_ref,
    acc_ref,
    max_ref,
    sum_ref,
):
    block = pl.program_id(0)
    me = lax.axis_index("seq")
    per_group = H // KVH
    kv_here = k_ref.shape[1] // DH
    rows = per_group * BLK
    scaling = DH ** (-0.5)

    def scan_entry(e, found):
        slot = slot_ref[near_ref[block, e]]
        list_ref[found] = lax.rem(slot, store_blocks)
        return found + (slot // store_blocks == me).astype(jnp.int32)

    found = lax.fori_loop(0, count_ref[block], scan_entry, jnp.int32(0))
    home = block // local_blocks == me

    @pl.when(jnp.logical_and(found == 0, jnp.logical_not(home)))
    def _():
        o_ref[...] = jnp.zeros_like(o_ref)
        lse_ref[...] = jnp.full_like(lse_ref, NEG)

    @pl.when(jnp.logical_or(found > 0, home))
    def _():
        def group_queries(g):
            return jnp.concatenate(
                [q_ref[:, (g * per_group + r) * DH : (g * per_group + r + 1) * DH] for r in range(per_group)],
                axis=0,
            )

        def scores_of(g, keys):
            return (
                lax.dot_general(
                    group_queries(g), keys, (((1,), (1,)), ((), ())), preferred_element_type=jnp.float32
                )
                * scaling
            )

        @pl.when(home)
        def _():
            start = pl.multiple_of(lax.rem(block, local_blocks) * BLK, BLK)
            position = lax.rem(lax.broadcasted_iota(jnp.int32, (rows, BLK), 0), BLK)
            causal = position >= lax.broadcasted_iota(jnp.int32, (rows, BLK), 1)
            for g in range(kv_here):
                cols = slice(g * DH, (g + 1) * DH)
                s = jnp.where(causal, scores_of(g, sk_ref[pl.ds(start, BLK), cols]), NEG)
                m = jnp.max(s, axis=-1, keepdims=True)
                p = jnp.exp(s - m)
                max_ref[g] = jnp.broadcast_to(m, (rows, BLK))
                sum_ref[g] = jnp.broadcast_to(jnp.sum(p, axis=-1, keepdims=True), (rows, BLK))
                acc_ref[g] = jnp.dot(
                    p.astype(jnp.bfloat16), sv_ref[pl.ds(start, BLK), cols], preferred_element_type=jnp.float32
                )

        @pl.when(jnp.logical_not(home))
        def _():
            max_ref[...] = jnp.full_like(max_ref, NEG)
            sum_ref[...] = jnp.zeros_like(sum_ref)
            acc_ref[...] = jnp.zeros_like(acc_ref)

        @pl.loop(0, found)
        def _(i):
            start = pl.multiple_of(list_ref[i] * BLK, BLK)
            for g in range(kv_here):
                cols = slice(g * DH, (g + 1) * DH)
                s = scores_of(g, k_ref[pl.ds(start, BLK), cols])
                old = max_ref[g]
                new = jnp.maximum(old, jnp.max(s, axis=-1, keepdims=True))
                p = jnp.exp(s - new)
                shrink = jnp.exp(old - new)
                max_ref[g] = new
                sum_ref[g] = sum_ref[g] * shrink + jnp.sum(p, axis=-1, keepdims=True)
                acc_ref[g] = acc_ref[g] * shrink + jnp.dot(
                    p.astype(jnp.bfloat16), v_ref[pl.ds(start, BLK), cols], preferred_element_type=jnp.float32
                )

        lane = lax.broadcasted_iota(jnp.int32, (BLK, BLK), 1)
        tile = jnp.full((BLK, BLK), NEG, jnp.float32)
        for g in range(kv_here):
            total = sum_ref[g]
            normal = (acc_ref[g] / total).astype(jnp.bfloat16)
            lse = max_ref[g] + jnp.log(total)
            for r in range(per_group):
                h = g * per_group + r
                o_ref[:, h * DH : (h + 1) * DH] = normal[r * BLK : (r + 1) * BLK]
                tile = jnp.where(lane == h, lse[r * BLK : (r + 1) * BLK], tile)
        lse_ref[...] = jnp.transpose(tile)[: lse_ref.shape[0]]


def return_kernel(n, heads, o_ref, lse_ref, out_ref, got, got_lse, send_sem, recv_sem, lsend_sem, lrecv_sem, own_sem):
    me = lax.axis_index("seq")
    rows = out_ref.shape[0]
    srows = got_lse.shape[1]
    blocks = rows // BLK
    barrier = pltpu.get_barrier_semaphore()
    for k in range(1, n):
        pl.semaphore_signal(barrier, inc=1, device_id={"seq": lax.rem(me + k, n)}, device_id_type=MESH)
    own = pltpu.make_async_copy(o_ref.at[pl.ds(pl.multiple_of(me * rows, rows), rows)], got.at[0], own_sem.at[0])
    own.start()
    own_lse = pltpu.make_async_copy(
        lse_ref.at[pl.ds(pl.multiple_of(me * srows, srows), srows)], got_lse.at[0], own_sem.at[1]
    )
    own_lse.start()
    pl.semaphore_wait(barrier, n - 1)
    copies = []
    for k in range(1, n):
        to = lax.rem(me + k, n)
        copies.append(
            pltpu.make_async_remote_copy(
                src_ref=lse_ref.at[pl.ds(pl.multiple_of(to * srows, srows), srows)],
                dst_ref=got_lse.at[k],
                send_sem=lsend_sem.at[k],
                recv_sem=lrecv_sem.at[k],
                device_id={"seq": to},
                device_id_type=MESH,
            )
        )
        copies.append(
            pltpu.make_async_remote_copy(
                src_ref=o_ref.at[pl.ds(pl.multiple_of(to * rows, rows), rows)],
                dst_ref=got.at[k],
                send_sem=send_sem.at[k],
                recv_sem=recv_sem.at[k],
                device_id={"seq": to},
                device_id_type=MESH,
            )
        )
    for copy in copies:
        copy.start()
    own.wait()
    own_lse.wait()
    for copy in copies:
        copy.wait()
    for b in range(blocks):
        at = slice(b * heads, (b + 1) * heads)

        def peak(i, top):
            return jnp.maximum(top, got_lse[i, at])

        top = lax.fori_loop(1, n, peak, got_lse[0, at])

        def total_of(i, total):
            return total + jnp.exp(got_lse[i, at] - top)

        total = lax.fori_loop(1, n, total_of, jnp.exp(got_lse[0, at] - top))

        def share(i):
            part = jnp.exp(got_lse[i, at] - top) / total
            padded = jnp.concatenate([part, jnp.zeros((BLK - heads, BLK), jnp.float32)], axis=0)
            return jnp.transpose(padded)

        lines = slice(b * BLK, (b + 1) * BLK)

        def add(i, sums):
            weight = share(i)
            return tuple(
                sums[h]
                + got[i, lines, h * DH : (h + 1) * DH].astype(jnp.float32)
                * jnp.broadcast_to(weight[:, h : h + 1], (BLK, DH))
                for h in range(heads)
            )

        sums = lax.fori_loop(0, n, add, tuple(jnp.zeros((BLK, DH), jnp.float32) for _ in range(heads)))
        for h in range(heads):
            out_ref[lines, h * DH : (h + 1) * DH] = sums[h].astype(jnp.bfloat16)


def body(
    queries,
    self_keys,
    self_values,
    store_keys,
    store_values,
    kv_slot,
    neighbours,
    counts,
    out_weight,
):
    n = lax.axis_size("seq")
    local_blocks, degree = neighbours.shape
    width = queries.shape[1]
    heads = width // DH
    store_blocks = store_keys.shape[0] // BLK
    all_blocks = local_blocks * n
    kv_here = store_keys.shape[1] // DH
    rows = (H // KVH) * BLK
    lists = jnp.concatenate([neighbours, counts[:, None]], axis=1)
    lists = lax.all_gather(lists, "seq", axis=0, tiled=True)
    all_queries = lax.all_gather(queries, "seq", axis=0, tiled=True)
    weight = lax.all_gather(out_weight, "seq", axis=1, tiled=True)
    smem = pl.BlockSpec(memory_space=pltpu.SMEM)

    def whole(a):
        return pl.BlockSpec(a.shape, lambda i: (0, 0))

    parts, lse = pl.pallas_call(
        functools.partial(part_kernel, local_blocks, store_blocks),
        grid=(all_blocks,),
        in_specs=[smem, smem, smem, pl.BlockSpec((BLK, width), lambda i: (i, 0))]
        + [whole(a) for a in (self_keys, self_values, store_keys, store_values)],
        out_specs=[
            pl.BlockSpec((BLK, width), lambda i: (i, 0)),
            pl.BlockSpec((heads, BLK), lambda i: (i, 0)),
        ],
        out_shape=[
            jax.ShapeDtypeStruct((all_blocks * BLK, width), jnp.bfloat16),
            jax.ShapeDtypeStruct((all_blocks * heads, BLK), jnp.float32),
        ],
        scratch_shapes=[
            pltpu.SMEM((degree + 1,), jnp.int32),
            pltpu.VMEM((kv_here, rows, DH), jnp.float32),
            pltpu.VMEM((kv_here, rows, BLK), jnp.float32),
            pltpu.VMEM((kv_here, rows, BLK), jnp.float32),
        ],
        compiler_params=pltpu.CompilerParams(vmem_limit_bytes=40 << 20),
        cost_estimate=pl.CostEstimate(flops=2_000_000_000, bytes_accessed=12 << 20, transcendentals=4_000_000),
    )(
        kv_slot,
        lists[:, :degree],
        lists[:, degree],
        all_queries,
        self_keys,
        self_values,
        store_keys,
        store_values,
    )
    local_rows = queries.shape[0]
    attended = pl.pallas_call(
        functools.partial(return_kernel, n, heads),
        in_specs=[pl.BlockSpec(memory_space=pl.ANY)] * 2,
        out_specs=pl.BlockSpec(memory_space=pltpu.VMEM),
        out_shape=jax.ShapeDtypeStruct((local_rows, width), jnp.bfloat16),
        scratch_shapes=[
            pltpu.VMEM((n, local_rows, width), jnp.bfloat16),
            pltpu.VMEM((n, local_blocks * heads, BLK), jnp.float32),
            pltpu.SemaphoreType.DMA((n,)),
            pltpu.SemaphoreType.DMA((n,)),
            pltpu.SemaphoreType.DMA((n,)),
            pltpu.SemaphoreType.DMA((n,)),
            pltpu.SemaphoreType.DMA((2,)),
        ],
        compiler_params=pltpu.CompilerParams(
            collective_id=0, has_side_effects=True, vmem_limit_bytes=50 << 20
        ),
        cost_estimate=pl.CostEstimate(flops=80_000_000, bytes_accessed=80 << 20, transcendentals=0),
    )(parts, lse)
    partial_value = jnp.dot(attended, weight, preferred_element_type=jnp.float32)
    return lax.psum_scatter(
        partial_value.astype(jnp.bfloat16), "head", scatter_dimension=0, tiled=True
    )


def solution(mesh):
    placed = (
        P("seq", "head"),
        P("seq", "head"),
        P("seq", "head"),
        P("seq", "head"),
        P("seq", "head"),
        P(),
        P("seq", None),
        P("seq"),
        P("head", "seq"),
    )
    return jax.shard_map(
        body, mesh=mesh, in_specs=placed, out_specs=P(("seq", "head"), None), check_vma=False
    )
```

```python
import functools

import jax
import jax.numpy as jnp
from jax import lax
from jax.experimental import pallas as pl
from jax.experimental.pallas import tpu as pltpu
from jax.sharding import PartitionSpec as P

H = 32
KVH = 8
DH = 128
BLK = 128
NEG = -1e30
STAT = 8
MESH = pl.DeviceIdType.MESH


def part_kernel(
    local_blocks,
    store_blocks,
    slot_ref,
    near_ref,
    count_ref,
    q_ref,
    sk_ref,
    sv_ref,
    k_ref,
    v_ref,
    o_ref,
    lse_ref,
    list_ref,
    acc_ref,
    max_ref,
    sum_ref,
):
    block = pl.program_id(0)
    me = lax.axis_index("seq")
    per_group = H // KVH
    kv_here = k_ref.shape[1] // DH
    rows = per_group * BLK
    scaling = DH ** (-0.5)

    def scan_entry(e, found):
        slot = slot_ref[near_ref[block, e]]
        list_ref[found] = lax.rem(slot, store_blocks)
        return found + (slot // store_blocks == me).astype(jnp.int32)

    found = lax.fori_loop(0, count_ref[block], scan_entry, jnp.int32(0))
    home = block // local_blocks == me

    @pl.when(jnp.logical_and(found == 0, jnp.logical_not(home)))
    def _():
        o_ref[...] = jnp.zeros_like(o_ref)
        lse_ref[...] = jnp.full_like(lse_ref, NEG)

    @pl.when(jnp.logical_or(found > 0, home))
    def _():
        def group_queries(g):
            return jnp.concatenate(
                [q_ref[:, (g * per_group + r) * DH : (g * per_group + r + 1) * DH] for r in range(per_group)],
                axis=0,
            )

        def scores_of(g, keys):
            return (
                lax.dot_general(
                    group_queries(g), keys, (((1,), (1,)), ((), ())), preferred_element_type=jnp.float32
                )
                * scaling
            )

        @pl.when(home)
        def _():
            start = pl.multiple_of(lax.rem(block, local_blocks) * BLK, BLK)
            position = lax.rem(lax.broadcasted_iota(jnp.int32, (rows, BLK), 0), BLK)
            causal = position >= lax.broadcasted_iota(jnp.int32, (rows, BLK), 1)
            for g in range(kv_here):
                cols = slice(g * DH, (g + 1) * DH)
                s = jnp.where(causal, scores_of(g, sk_ref[pl.ds(start, BLK), cols]), NEG)
                m = jnp.max(s, axis=-1, keepdims=True)
                p = jnp.exp(s - m)
                max_ref[g] = jnp.broadcast_to(m, (rows, BLK))
                sum_ref[g] = jnp.broadcast_to(jnp.sum(p, axis=-1, keepdims=True), (rows, BLK))
                acc_ref[g] = jnp.dot(
                    p.astype(jnp.bfloat16), sv_ref[pl.ds(start, BLK), cols], preferred_element_type=jnp.float32
                )

        @pl.when(jnp.logical_not(home))
        def _():
            max_ref[...] = jnp.full_like(max_ref, NEG)
            sum_ref[...] = jnp.zeros_like(sum_ref)
            acc_ref[...] = jnp.zeros_like(acc_ref)

        @pl.loop(0, found)
        def _(i):
            start = pl.multiple_of(list_ref[i] * BLK, BLK)
            for g in range(kv_here):
                cols = slice(g * DH, (g + 1) * DH)
                s = scores_of(g, k_ref[pl.ds(start, BLK), cols])
                old = max_ref[g]
                new = jnp.maximum(old, jnp.max(s, axis=-1, keepdims=True))
                p = jnp.exp(s - new)
                shrink = jnp.exp(old - new)
                max_ref[g] = new
                sum_ref[g] = sum_ref[g] * shrink + jnp.sum(p, axis=-1, keepdims=True)
                acc_ref[g] = acc_ref[g] * shrink + jnp.dot(
                    p.astype(jnp.bfloat16), v_ref[pl.ds(start, BLK), cols], preferred_element_type=jnp.float32
                )

        lane = lax.broadcasted_iota(jnp.int32, (BLK, BLK), 1)
        for g in range(kv_here):
            total = sum_ref[g]
            normal = (acc_ref[g] / total).astype(jnp.bfloat16)
            lse = max_ref[g] + jnp.log(total)
            tile = jnp.full((BLK, BLK), NEG, jnp.float32)
            for r in range(per_group):
                o_ref[0, g, :, r * DH : (r + 1) * DH] = normal[r * BLK : (r + 1) * BLK]
                tile = jnp.where(lane == r, lse[r * BLK : (r + 1) * BLK], tile)
            lse_ref[0, g] = jnp.transpose(tile)[:STAT]


def ring_place(index, n):
    odd = lax.rem(index, 2)
    half = index // 2
    return (1 - odd) * half + odd * (n - 1 - half)


def ring_index(place, n):
    place = lax.rem(place + 2 * n, n)
    far = place // (n // 2)
    return (1 - far) * (2 * place) + far * (2 * (n - 1 - place) + 1)


def gather_kernel(n, pieces, with_table, *refs):
    if with_table:
        x_ref, table_ref, out_ref, tables_ref, own_sem, send_sem, recv_sem, tsend_sem, trecv_sem = refs
    else:
        x_ref, out_ref, own_sem, send_sem, recv_sem = refs
    me = lax.axis_index("seq")
    place = ring_place(me, n)
    rows = x_ref.shape[0]
    sub = rows // pieces
    half = n // 2
    ways = (1, -1)
    beside = [ring_index(place + way, n) for way in ways]
    barrier = pltpu.get_barrier_semaphore()
    if with_table:
        for k in range(1, n):
            pl.semaphore_signal(barrier, inc=1, device_id={"seq": lax.rem(me + k, n)}, device_id_type=MESH)
    else:
        for other in beside:
            pl.semaphore_signal(barrier, inc=1, device_id={"seq": other}, device_id_type=MESH)
    own = pltpu.make_async_copy(x_ref, out_ref.at[pl.ds(pl.multiple_of(me * rows, rows), rows)], own_sem.at[0])
    own.start()
    pl.semaphore_wait(barrier, n - 1 if with_table else 2)

    def copy(way, step, piece):
        owner = ring_index(place - ways[way] * step, n)
        there = pl.ds(pl.multiple_of(owner * rows + piece * sub, sub), sub)
        source = x_ref.at[pl.ds(piece * sub, sub)] if step == 0 else out_ref.at[there]
        return pltpu.make_async_remote_copy(
            src_ref=source,
            dst_ref=out_ref.at[there],
            send_sem=send_sem.at[way, step, piece],
            recv_sem=recv_sem.at[way, step, piece],
            device_id={"seq": beside[way]},
            device_id_type=MESH,
        )

    table_copies = []
    if with_table:
        tables_ref[pl.ds(me, 1)] = table_ref[...][None]
        for k in range(1, n):
            table_copies.append(
                pltpu.make_async_remote_copy(
                    src_ref=table_ref,
                    dst_ref=tables_ref.at[me],
                    send_sem=tsend_sem.at[k],
                    recv_sem=trecv_sem.at[k],
                    device_id={"seq": lax.rem(me + k, n)},
                    device_id_type=MESH,
                )
            )
        for one in table_copies:
            one.start()
    started = []
    for step in range(half):
        for spot in range(pieces):
            for way in range(2):
                piece = spot if way == 0 else pieces - 1 - spot
                if step > 0:
                    copy(way, step - 1, piece).wait_recv()
                if step < half - 1 or spot < pieces // 2:
                    one = copy(way, step, piece)
                    one.start()
                    started.append(one)
    for spot in range(pieces // 2):
        for way in range(2):
            copy(way, half - 1, spot if way == 0 else pieces - 1 - spot).wait_recv()
    for one in started:
        one.wait_send()
    for one in table_copies:
        one.wait()
    own.wait()


def gathered(x, n, pieces, number, table=None):
    rows, width = x.shape
    with_table = table is not None
    vmem = pl.BlockSpec(memory_space=pltpu.VMEM)
    out_shape = [jax.ShapeDtypeStruct((n * rows, width), x.dtype)]
    scratch = [
        pltpu.SemaphoreType.DMA((1,)),
        pltpu.SemaphoreType.DMA((2, n // 2, pieces)),
        pltpu.SemaphoreType.DMA((2, n // 2, pieces)),
    ]
    if with_table:
        out_shape.append(jax.ShapeDtypeStruct((n,) + table.shape, table.dtype))
        scratch += [pltpu.SemaphoreType.DMA((n,)), pltpu.SemaphoreType.DMA((n,))]
    return pl.pallas_call(
        functools.partial(gather_kernel, n, pieces, with_table),
        in_specs=[vmem] * (1 + with_table),
        out_specs=[vmem] * (1 + with_table),
        out_shape=out_shape,
        scratch_shapes=scratch,
        compiler_params=pltpu.CompilerParams(
            collective_id=number, has_side_effects=True, vmem_limit_bytes=50 << 20
        ),
    )(*([x, table] if with_table else [x]))


def merge(lse_a, lse_b):
    top = jnp.maximum(lse_a, lse_b)
    a = jnp.exp(lse_a - top)
    b = jnp.exp(lse_b - top)
    total = a + b
    both = jnp.concatenate([a / total, b / total, jnp.zeros((BLK - 2 * STAT, BLK), jnp.float32)], axis=0)
    return jnp.transpose(both), top + jnp.log(total)


def reduce_kernel(n, o_ref, lse_ref, out_ref, got, got_lse, own, own_sem, send_sem, recv_sem, lsend_sem, lrecv_sem):
    me = lax.axis_index("seq")
    place = ring_place(me, n)
    groups, width = got.shape[2], got.shape[4]
    ways = (1, -1)
    beside = [ring_index(place + way, n) for way in ways]
    barrier = pltpu.get_barrier_semaphore()
    for other in beside:
        pl.semaphore_signal(barrier, inc=1, device_id={"seq": other}, device_id_type=MESH)

    def home(way, step):
        return ring_index(place - ways[way] * (1 + step), n)

    def fetch(way, step):
        return pltpu.make_async_copy(
            o_ref.at[home(way, step) * 2 + way], own.at[way, lax.rem(step, 2)], own_sem.at[way, lax.rem(step, 2)]
        )

    def copies(way, step, g, before):
        at = home(way, step) * 2 + way
        first = before is None
        return (
            pltpu.make_async_remote_copy(
                src_ref=lse_ref.at[at, g] if first else got_lse.at[way, before, g],
                dst_ref=got_lse.at[way, step, g],
                send_sem=lsend_sem.at[way, step, g],
                recv_sem=lrecv_sem.at[way, step, g],
                device_id={"seq": beside[way]},
                device_id_type=MESH,
            ),
            pltpu.make_async_remote_copy(
                src_ref=o_ref.at[at, g] if first else got.at[way, before, g],
                dst_ref=got.at[way, step, g],
                send_sem=send_sem.at[way, step, g],
                recv_sem=recv_sem.at[way, step, g],
                device_id={"seq": beside[way]},
                device_id_type=MESH,
            ),
        )

    def merged(way, step, g):
        for one in copies(way, step - 1, g, step - 1):
            one.wait_recv()
        if g == 0:
            fetch(way, step).wait()
        at = home(way, step) * 2 + way
        shares, lse = merge(got_lse[way, step - 1, g], lse_ref[at, g])
        columns = []
        for r in range(width // DH):
            cols = slice(r * DH, (r + 1) * DH)
            columns.append(
                got[way, step - 1, g, :, cols].astype(jnp.float32) * shares[:, r : r + 1]
                + own[way, lax.rem(step, 2), g, :, cols].astype(jnp.float32) * shares[:, STAT + r : STAT + r + 1]
            )
        return columns, lse

    for way in range(2):
        fetch(way, 1).start()
    pl.semaphore_wait(barrier, 2)
    for g in range(groups):
        for way in range(2):
            for one in copies(way, 0, g, None):
                one.start()

    def one_step(step, carry):
        for way in range(2):
            fetch(way, step + 1).start()
        for g in range(groups):
            for way in range(2):
                columns, lse = merged(way, step, g)
                got_lse[way, step - 1, g] = lse
                for r, value in enumerate(columns):
                    got[way, step - 1, g, :, r * DH : (r + 1) * DH] = value.astype(jnp.bfloat16)
            for way in range(2):
                for one in copies(way, step, g, step - 1):
                    one.start()
        return carry

    lax.fori_loop(1, n - 1, one_step, 0)
    for g in range(groups):
        for way in range(2):
            columns, _ = merged(way, n - 1, g)
            for r, value in enumerate(columns):
                at = g * width + r * DH
                out_ref[way * BLK : (way + 1) * BLK, at : at + DH] = value.astype(jnp.bfloat16)
    for g in range(groups):
        for way in range(2):
            for one in copies(way, 0, g, None):
                one.wait_send()

    def drain(step, carry):
        for g in range(groups):
            for way in range(2):
                for one in copies(way, step, g, step - 1):
                    one.wait_send()
        return carry

    lax.fori_loop(1, n - 1, drain, 0)


def body(
    queries,
    self_keys,
    self_values,
    store_keys,
    store_values,
    kv_slot,
    neighbours,
    counts,
    out_weight,
):
    n = lax.axis_size("seq")
    head_count = lax.axis_size("head")
    local_blocks, degree = neighbours.shape
    local_rows, width = queries.shape
    store_blocks = store_keys.shape[0] // BLK
    all_blocks = local_blocks * n
    kv_here = store_keys.shape[1] // DH
    group_width = (H // KVH) * DH
    rows = (H // KVH) * BLK
    table = jnp.concatenate([neighbours, counts[:, None]], axis=1)
    table = jnp.pad(table, ((0, 8 - local_blocks), (0, 2 * BLK - table.shape[1] - BLK)))
    all_queries, tables = gathered(queries, n, 2, 0, table)
    near = tables[:, :local_blocks, :degree].reshape(all_blocks, degree)
    count = tables[:, :local_blocks, degree].reshape(all_blocks)
    smem = pl.BlockSpec(memory_space=pltpu.SMEM)

    def whole(a):
        return pl.BlockSpec(a.shape, lambda i: (0, 0))

    parts, lse = pl.pallas_call(
        functools.partial(part_kernel, local_blocks, store_blocks),
        grid=(all_blocks,),
        in_specs=[smem, smem, smem, pl.BlockSpec((BLK, width), lambda i: (i, 0))]
        + [whole(a) for a in (self_keys, self_values, store_keys, store_values)],
        out_specs=[
            pl.BlockSpec((1, kv_here, BLK, group_width), lambda i: (i, 0, 0, 0)),
            pl.BlockSpec((1, kv_here, STAT, BLK), lambda i: (i, 0, 0, 0)),
        ],
        out_shape=[
            jax.ShapeDtypeStruct((all_blocks, kv_here, BLK, group_width), jnp.bfloat16),
            jax.ShapeDtypeStruct((all_blocks, kv_here, STAT, BLK), jnp.float32),
        ],
        scratch_shapes=[
            pltpu.SMEM((degree + 1,), jnp.int32),
            pltpu.VMEM((kv_here, rows, DH), jnp.float32),
            pltpu.VMEM((kv_here, rows, BLK), jnp.float32),
            pltpu.VMEM((kv_here, rows, BLK), jnp.float32),
        ],
        compiler_params=pltpu.CompilerParams(vmem_limit_bytes=40 << 20),
        cost_estimate=pl.CostEstimate(flops=2_000_000_000, bytes_accessed=12 << 20, transcendentals=4_000_000),
    )(kv_slot, near, count, all_queries, self_keys, self_values, store_keys, store_values)
    dma = pltpu.SemaphoreType.DMA((2, n - 1, kv_here))
    attended = pl.pallas_call(
        functools.partial(reduce_kernel, n),
        in_specs=[pl.BlockSpec(memory_space=pl.ANY), pl.BlockSpec(memory_space=pltpu.VMEM)],
        out_specs=pl.BlockSpec(memory_space=pltpu.VMEM),
        out_shape=jax.ShapeDtypeStruct((local_rows, width), jnp.bfloat16),
        scratch_shapes=[
            pltpu.VMEM((2, n - 1, kv_here, BLK, group_width), jnp.bfloat16),
            pltpu.VMEM((2, n - 1, kv_here, STAT, BLK), jnp.float32),
            pltpu.VMEM((2, 2, kv_here, BLK, group_width), jnp.bfloat16),
            pltpu.SemaphoreType.DMA((2, 2)),
            dma,
            dma,
            dma,
            dma,
        ],
        compiler_params=pltpu.CompilerParams(
            collective_id=1, has_side_effects=True, vmem_limit_bytes=50 << 20
        ),
    )(parts, lse)
    (all_attended,) = gathered(attended, n, 2, 2)
    partial_value = jnp.dot(all_attended, out_weight, preferred_element_type=jnp.float32).astype(jnp.bfloat16)
    columns = out_weight.shape[1]
    share = local_rows // head_count
    split = partial_value.reshape(n, head_count, share, columns).transpose(1, 0, 2, 3)
    summed = lax.psum_scatter(split.reshape(head_count * n * share, columns), "head", scatter_dimension=0, tiled=True)
    summed = summed.reshape(n, share, columns)
    swapped = lax.all_to_all(summed, "seq", split_axis=0, concat_axis=0, tiled=True)
    return jnp.transpose(swapped, (1, 0, 2)).reshape(share, n * columns)


def solution(mesh):
    placed = (
        P("seq", "head"),
        P("seq", "head"),
        P("seq", "head"),
        P("seq", "head"),
        P("seq", "head"),
        P(),
        P("seq", None),
        P("seq"),
        P("head", "seq"),
    )
    return jax.shard_map(
        body, mesh=mesh, in_specs=placed, out_specs=P(("seq", "head"), None), check_vma=False
    )
```

```python
import functools

import jax
import jax.numpy as jnp
from jax import lax
from jax.experimental import pallas as pl
from jax.experimental.pallas import tpu as pltpu
from jax.sharding import PartitionSpec as P

H = 32
KVH = 8
DH = 128
BLK = 128
NEG = -1e30
STAT = 8
MESH = pl.DeviceIdType.MESH


def part_kernel(
    local_blocks,
    store_blocks,
    slot_ref,
    near_ref,
    count_ref,
    q_ref,
    sk_ref,
    sv_ref,
    k_ref,
    v_ref,
    o_ref,
    lse_ref,
    list_ref,
    acc_ref,
    max_ref,
    sum_ref,
):
    block = pl.program_id(0)
    me = lax.axis_index("seq")
    per_group = H // KVH
    kv_here = k_ref.shape[1] // DH
    rows = per_group * BLK
    scaling = DH ** (-0.5)

    def scan_entry(e, found):
        slot = slot_ref[near_ref[block, e]]
        list_ref[found] = lax.rem(slot, store_blocks)
        return found + (slot // store_blocks == me).astype(jnp.int32)

    found = lax.fori_loop(0, count_ref[block], scan_entry, jnp.int32(0))
    home = block // local_blocks == me

    @pl.when(jnp.logical_and(found == 0, jnp.logical_not(home)))
    def _():
        o_ref[...] = jnp.zeros_like(o_ref)
        lse_ref[...] = jnp.full_like(lse_ref, NEG)

    @pl.when(jnp.logical_or(found > 0, home))
    def _():
        def group_queries(g):
            return jnp.concatenate(
                [q_ref[:, (g * per_group + r) * DH : (g * per_group + r + 1) * DH] for r in range(per_group)],
                axis=0,
            )

        def scores_of(g, keys):
            return (
                lax.dot_general(
                    group_queries(g), keys, (((1,), (1,)), ((), ())), preferred_element_type=jnp.float32
                )
                * scaling
            )

        @pl.when(home)
        def _():
            start = pl.multiple_of(lax.rem(block, local_blocks) * BLK, BLK)
            position = lax.rem(lax.broadcasted_iota(jnp.int32, (rows, BLK), 0), BLK)
            causal = position >= lax.broadcasted_iota(jnp.int32, (rows, BLK), 1)
            for g in range(kv_here):
                cols = slice(g * DH, (g + 1) * DH)
                s = jnp.where(causal, scores_of(g, sk_ref[pl.ds(start, BLK), cols]), NEG)
                m = jnp.max(s, axis=-1, keepdims=True)
                p = jnp.exp(s - m)
                max_ref[g] = jnp.broadcast_to(m, (rows, BLK))
                sum_ref[g] = jnp.broadcast_to(jnp.sum(p, axis=-1, keepdims=True), (rows, BLK))
                acc_ref[g] = jnp.dot(
                    p.astype(jnp.bfloat16), sv_ref[pl.ds(start, BLK), cols], preferred_element_type=jnp.float32
                )

        @pl.when(jnp.logical_not(home))
        def _():
            max_ref[...] = jnp.full_like(max_ref, NEG)
            sum_ref[...] = jnp.zeros_like(sum_ref)
            acc_ref[...] = jnp.zeros_like(acc_ref)

        @pl.loop(0, found)
        def _(i):
            start = pl.multiple_of(list_ref[i] * BLK, BLK)
            for g in range(kv_here):
                cols = slice(g * DH, (g + 1) * DH)
                s = scores_of(g, k_ref[pl.ds(start, BLK), cols])
                old = max_ref[g]
                new = jnp.maximum(old, jnp.max(s, axis=-1, keepdims=True))
                p = jnp.exp(s - new)
                shrink = jnp.exp(old - new)
                max_ref[g] = new
                sum_ref[g] = sum_ref[g] * shrink + jnp.sum(p, axis=-1, keepdims=True)
                acc_ref[g] = acc_ref[g] * shrink + jnp.dot(
                    p.astype(jnp.bfloat16), v_ref[pl.ds(start, BLK), cols], preferred_element_type=jnp.float32
                )

        lane = lax.broadcasted_iota(jnp.int32, (BLK, BLK), 1)
        for g in range(kv_here):
            total = sum_ref[g]
            normal = (acc_ref[g] / total).astype(jnp.bfloat16)
            lse = max_ref[g] + jnp.log(total)
            tile = jnp.full((BLK, BLK), NEG, jnp.float32)
            for r in range(per_group):
                o_ref[0, g, :, r * DH : (r + 1) * DH] = normal[r * BLK : (r + 1) * BLK]
                tile = jnp.where(lane == r, lse[r * BLK : (r + 1) * BLK], tile)
            lse_ref[0, g] = jnp.transpose(tile)[:STAT]


def ring_place(index, n):
    odd = lax.rem(index, 2)
    half = index // 2
    return (1 - odd) * half + odd * (n - 1 - half)


def ring_index(place, n):
    place = lax.rem(place + 2 * n, n)
    far = place // (n // 2)
    return (1 - far) * (2 * place) + far * (2 * (n - 1 - place) + 1)


def gather_kernel(n, pieces, with_table, *refs):
    if with_table:
        x_ref, table_ref, out_ref, tables_ref, own_sem, send_sem, recv_sem, tsend_sem, trecv_sem = refs
    else:
        x_ref, out_ref, own_sem, send_sem, recv_sem = refs
    me = lax.axis_index("seq")
    place = ring_place(me, n)
    rows = x_ref.shape[0]
    sub = rows // pieces
    half = n // 2
    ways = (1, -1)
    beside = [ring_index(place + way, n) for way in ways]
    barrier = pltpu.get_barrier_semaphore()
    if with_table:
        for k in range(1, n):
            pl.semaphore_signal(barrier, inc=1, device_id={"seq": lax.rem(me + k, n)}, device_id_type=MESH)
    else:
        for other in beside:
            pl.semaphore_signal(barrier, inc=1, device_id={"seq": other}, device_id_type=MESH)
    own = pltpu.make_async_copy(x_ref, out_ref.at[pl.ds(pl.multiple_of(me * rows, rows), rows)], own_sem.at[0])
    own.start()
    pl.semaphore_wait(barrier, n - 1 if with_table else 2)

    def copy(way, step, piece):
        owner = ring_index(place - ways[way] * step, n)
        there = pl.ds(pl.multiple_of(owner * rows + piece * sub, sub), sub)
        source = x_ref.at[pl.ds(piece * sub, sub)] if step == 0 else out_ref.at[there]
        return pltpu.make_async_remote_copy(
            src_ref=source,
            dst_ref=out_ref.at[there],
            send_sem=send_sem.at[way, step, piece],
            recv_sem=recv_sem.at[way, step, piece],
            device_id={"seq": beside[way]},
            device_id_type=MESH,
        )

    table_copies = []
    if with_table:
        tables_ref[pl.ds(me, 1)] = table_ref[...][None]
        for k in range(1, n):
            table_copies.append(
                pltpu.make_async_remote_copy(
                    src_ref=table_ref,
                    dst_ref=tables_ref.at[me],
                    send_sem=tsend_sem.at[k],
                    recv_sem=trecv_sem.at[k],
                    device_id={"seq": lax.rem(me + k, n)},
                    device_id_type=MESH,
                )
            )
        for one in table_copies:
            one.start()
    started = []
    for step in range(half):
        for spot in range(pieces):
            for way in range(2):
                piece = spot if way == 0 else pieces - 1 - spot
                if step > 0:
                    copy(way, step - 1, piece).wait_recv()
                if step < half - 1 or spot < pieces // 2:
                    one = copy(way, step, piece)
                    one.start()
                    started.append(one)
    for spot in range(pieces // 2):
        for way in range(2):
            copy(way, half - 1, spot if way == 0 else pieces - 1 - spot).wait_recv()
    for one in started:
        one.wait_send()
    for one in table_copies:
        one.wait()
    own.wait()


def gathered(x, n, pieces, number, table=None):
    rows, width = x.shape
    with_table = table is not None
    vmem = pl.BlockSpec(memory_space=pltpu.VMEM)
    out_shape = [jax.ShapeDtypeStruct((n * rows, width), x.dtype)]
    scratch = [
        pltpu.SemaphoreType.DMA((1,)),
        pltpu.SemaphoreType.DMA((2, n // 2, pieces)),
        pltpu.SemaphoreType.DMA((2, n // 2, pieces)),
    ]
    if with_table:
        out_shape.append(jax.ShapeDtypeStruct((n,) + table.shape, table.dtype))
        scratch += [pltpu.SemaphoreType.DMA((n,)), pltpu.SemaphoreType.DMA((n,))]
    return pl.pallas_call(
        functools.partial(gather_kernel, n, pieces, with_table),
        in_specs=[vmem] * (1 + with_table),
        out_specs=[vmem] * (1 + with_table),
        out_shape=out_shape,
        scratch_shapes=scratch,
        compiler_params=pltpu.CompilerParams(
            collective_id=number, has_side_effects=True, vmem_limit_bytes=50 << 20
        ),
    )(*([x, table] if with_table else [x]))


def merge(lse_a, lse_b):
    top = jnp.maximum(lse_a, lse_b)
    a = jnp.exp(lse_a - top)
    b = jnp.exp(lse_b - top)
    total = a + b
    both = jnp.concatenate([a / total, b / total, jnp.zeros((BLK - 2 * STAT, BLK), jnp.float32)], axis=0)
    return jnp.transpose(both), top + jnp.log(total)


def reduce_kernel(n, o_ref, lse_ref, out_ref, got, got_lse, own, own_sem, send_sem, recv_sem, lsend_sem, lrecv_sem):
    me = lax.axis_index("seq")
    place = ring_place(me, n)
    groups, width = got.shape[2], got.shape[4]
    ways = (1, -1)
    beside = [ring_index(place + way, n) for way in ways]
    barrier = pltpu.get_barrier_semaphore()
    for other in beside:
        pl.semaphore_signal(barrier, inc=1, device_id={"seq": other}, device_id_type=MESH)

    def home(way, step):
        return ring_index(place - ways[way] * (1 + step), n)

    def fetch(way, step):
        return pltpu.make_async_copy(
            o_ref.at[home(way, step) * 2 + way], own.at[way, lax.rem(step, 2)], own_sem.at[way, lax.rem(step, 2)]
        )

    def copies(way, step, g, before):
        at = home(way, step) * 2 + way
        first = before is None
        return (
            pltpu.make_async_remote_copy(
                src_ref=lse_ref.at[at, g] if first else got_lse.at[way, before, g],
                dst_ref=got_lse.at[way, step, g],
                send_sem=lsend_sem.at[way, step, g],
                recv_sem=lrecv_sem.at[way, step, g],
                device_id={"seq": beside[way]},
                device_id_type=MESH,
            ),
            pltpu.make_async_remote_copy(
                src_ref=o_ref.at[at, g] if first else got.at[way, before, g],
                dst_ref=got.at[way, step, g],
                send_sem=send_sem.at[way, step, g],
                recv_sem=recv_sem.at[way, step, g],
                device_id={"seq": beside[way]},
                device_id_type=MESH,
            ),
        )

    def merged(way, step, g):
        for one in copies(way, step - 1, g, step - 1):
            one.wait_recv()
        if g == 0:
            fetch(way, step).wait()
        at = home(way, step) * 2 + way
        shares, lse = merge(got_lse[way, step - 1, g], lse_ref[at, g])
        columns = []
        for r in range(width // DH):
            cols = slice(r * DH, (r + 1) * DH)
            columns.append(
                got[way, step - 1, g, :, cols].astype(jnp.float32) * shares[:, r : r + 1]
                + own[way, lax.rem(step, 2), g, :, cols].astype(jnp.float32) * shares[:, STAT + r : STAT + r + 1]
            )
        return columns, lse

    for way in range(2):
        fetch(way, 1).start()
    pl.semaphore_wait(barrier, 2)
    for g in range(groups):
        for way in range(2):
            for one in copies(way, 0, g, None):
                one.start()

    def one_step(step, carry):
        for way in range(2):
            fetch(way, step + 1).start()
        for g in range(groups):
            for way in range(2):
                columns, lse = merged(way, step, g)
                got_lse[way, step - 1, g] = lse
                for r, value in enumerate(columns):
                    got[way, step - 1, g, :, r * DH : (r + 1) * DH] = value.astype(jnp.bfloat16)
            for way in range(2):
                for one in copies(way, step, g, step - 1):
                    one.start()
        return carry

    lax.fori_loop(1, n - 1, one_step, 0)
    for g in range(groups):
        for way in range(2):
            columns, _ = merged(way, n - 1, g)
            for r, value in enumerate(columns):
                at = g * width + r * DH
                out_ref[way * BLK : (way + 1) * BLK, at : at + DH] = value.astype(jnp.bfloat16)
    for g in range(groups):
        for way in range(2):
            for one in copies(way, 0, g, None):
                one.wait_send()

    def drain(step, carry):
        for g in range(groups):
            for way in range(2):
                for one in copies(way, step, g, step - 1):
                    one.wait_send()
        return carry

    lax.fori_loop(1, n - 1, drain, 0)


def finish_kernel(n, heads, p_ref, out_ref, got, summed, landed, hsend, hrecv, send_sem, recv_sem):
    me = lax.axis_index("seq")
    mine = lax.axis_index("head")
    columns = p_ref.shape[3]
    barrier = pltpu.get_barrier_semaphore()
    for k in range(1, heads):
        pl.semaphore_signal(barrier, inc=1, device_id={"head": lax.rem(mine + k, heads)}, device_id_type=MESH)
    for k in range(1, n):
        pl.semaphore_signal(barrier, inc=1, device_id={"seq": lax.rem(me + k, n)}, device_id_type=MESH)
    pl.semaphore_wait(barrier, heads + n - 2)
    first = []
    for k in range(1, heads):
        to = lax.rem(mine + k, heads)
        first.append(
            pltpu.make_async_remote_copy(
                src_ref=p_ref.at[to],
                dst_ref=got.at[k],
                send_sem=hsend.at[k],
                recv_sem=hrecv.at[k],
                device_id={"head": to},
                device_id_type=MESH,
            )
        )
    for one in first:
        one.start()
    for one in first:
        one.wait()

    def add(i, carry):
        total = p_ref[mine, i].astype(jnp.float32)
        for k in range(1, heads):
            total = total + got[k, i].astype(jnp.float32)
        summed[i] = total.astype(jnp.bfloat16)
        return carry

    lax.fori_loop(0, n, add, 0)
    second = []
    for k in range(1, n):
        to = lax.rem(me + k, n)
        second.append(
            pltpu.make_async_remote_copy(
                src_ref=summed.at[to],
                dst_ref=landed.at[me],
                send_sem=send_sem.at[k],
                recv_sem=recv_sem.at[k],
                device_id={"seq": to},
                device_id_type=MESH,
            )
        )
    for one in second:
        one.start()
    landed[me] = summed[me]
    for one in second:
        one.wait()
    for i in range(n):
        out_ref[:, i * columns : (i + 1) * columns] = landed[i]


def finished(split):
    heads, n, share, columns = split.shape
    vmem = pl.BlockSpec(memory_space=pltpu.VMEM)
    return pl.pallas_call(
        functools.partial(finish_kernel, n, heads),
        in_specs=[vmem],
        out_specs=vmem,
        out_shape=jax.ShapeDtypeStruct((share, n * columns), split.dtype),
        scratch_shapes=[
            pltpu.VMEM(split.shape, split.dtype),
            pltpu.VMEM((n, share, columns), split.dtype),
            pltpu.VMEM((n, share, columns), split.dtype),
            pltpu.SemaphoreType.DMA((heads,)),
            pltpu.SemaphoreType.DMA((heads,)),
            pltpu.SemaphoreType.DMA((n,)),
            pltpu.SemaphoreType.DMA((n,)),
        ],
        compiler_params=pltpu.CompilerParams(
            collective_id=3, has_side_effects=True, vmem_limit_bytes=50 << 20
        ),
    )(split)


def body(
    queries,
    self_keys,
    self_values,
    store_keys,
    store_values,
    kv_slot,
    neighbours,
    counts,
    out_weight,
):
    n = lax.axis_size("seq")
    head_count = lax.axis_size("head")
    local_blocks, degree = neighbours.shape
    local_rows, width = queries.shape
    store_blocks = store_keys.shape[0] // BLK
    all_blocks = local_blocks * n
    kv_here = store_keys.shape[1] // DH
    group_width = (H // KVH) * DH
    rows = (H // KVH) * BLK
    table = jnp.concatenate([neighbours, counts[:, None]], axis=1)
    table = jnp.pad(table, ((0, 8 - local_blocks), (0, 2 * BLK - table.shape[1] - BLK)))
    all_queries, tables = gathered(queries, n, 2, 0, table)
    near = tables[:, :local_blocks, :degree].reshape(all_blocks, degree)
    count = tables[:, :local_blocks, degree].reshape(all_blocks)
    smem = pl.BlockSpec(memory_space=pltpu.SMEM)

    def whole(a):
        return pl.BlockSpec(a.shape, lambda i: (0, 0))

    parts, lse = pl.pallas_call(
        functools.partial(part_kernel, local_blocks, store_blocks),
        grid=(all_blocks,),
        in_specs=[smem, smem, smem, pl.BlockSpec((BLK, width), lambda i: (i, 0))]
        + [whole(a) for a in (self_keys, self_values, store_keys, store_values)],
        out_specs=[
            pl.BlockSpec((1, kv_here, BLK, group_width), lambda i: (i, 0, 0, 0)),
            pl.BlockSpec((1, kv_here, STAT, BLK), lambda i: (i, 0, 0, 0)),
        ],
        out_shape=[
            jax.ShapeDtypeStruct((all_blocks, kv_here, BLK, group_width), jnp.bfloat16),
            jax.ShapeDtypeStruct((all_blocks, kv_here, STAT, BLK), jnp.float32),
        ],
        scratch_shapes=[
            pltpu.SMEM((degree + 1,), jnp.int32),
            pltpu.VMEM((kv_here, rows, DH), jnp.float32),
            pltpu.VMEM((kv_here, rows, BLK), jnp.float32),
            pltpu.VMEM((kv_here, rows, BLK), jnp.float32),
        ],
        compiler_params=pltpu.CompilerParams(vmem_limit_bytes=40 << 20),
        cost_estimate=pl.CostEstimate(flops=2_000_000_000, bytes_accessed=12 << 20, transcendentals=4_000_000),
    )(kv_slot, near, count, all_queries, self_keys, self_values, store_keys, store_values)
    dma = pltpu.SemaphoreType.DMA((2, n - 1, kv_here))
    attended = pl.pallas_call(
        functools.partial(reduce_kernel, n),
        in_specs=[pl.BlockSpec(memory_space=pl.ANY), pl.BlockSpec(memory_space=pltpu.VMEM)],
        out_specs=pl.BlockSpec(memory_space=pltpu.VMEM),
        out_shape=jax.ShapeDtypeStruct((local_rows, width), jnp.bfloat16),
        scratch_shapes=[
            pltpu.VMEM((2, n - 1, kv_here, BLK, group_width), jnp.bfloat16),
            pltpu.VMEM((2, n - 1, kv_here, STAT, BLK), jnp.float32),
            pltpu.VMEM((2, 2, kv_here, BLK, group_width), jnp.bfloat16),
            pltpu.SemaphoreType.DMA((2, 2)),
            dma,
            dma,
            dma,
            dma,
        ],
        compiler_params=pltpu.CompilerParams(
            collective_id=1, has_side_effects=True, vmem_limit_bytes=50 << 20
        ),
    )(parts, lse)
    (all_attended,) = gathered(attended, n, 2, 2)
    partial_value = jnp.dot(all_attended, out_weight, preferred_element_type=jnp.float32).astype(jnp.bfloat16)
    columns = out_weight.shape[1]
    share = local_rows // head_count
    split = partial_value.reshape(n, head_count, share, columns).transpose(1, 0, 2, 3)
    return finished(split)


def solution(mesh):
    placed = (
        P("seq", "head"),
        P("seq", "head"),
        P("seq", "head"),
        P("seq", "head"),
        P("seq", "head"),
        P(),
        P("seq", None),
        P("seq"),
        P("head", "seq"),
    )
    return jax.shard_map(
        body, mesh=mesh, in_specs=placed, out_specs=P(("seq", "head"), None), check_vma=False
    )
```
